32 devices in a mesh: dp: 1 (over z), fsdp: 32 (over y, x, core).
Axes of the slice: x: 4, y: 4, z: 1, core: 2. Of those that a mesh axis runs over, the one named last changes fastest.
The devices are a block of a 4x4x8 slice.
Arguments:
- latents: bfloat16 [2048, 16, 1152], P(('dp', 'fsdp'))
- cond_emb: bfloat16 [2048, 1152], P(('dp', 'fsdp'))
- w_ada: bfloat16 [2, 1152, 6912], P(None, 'fsdp')
- b_ada: bfloat16 [2, 6912], replicated
- w_qkv: bfloat16 [2, 1152, 3456], P(None, 'fsdp')
- b_qkv: bfloat16 [2, 3456], replicated
- w_proj: bfloat16 [2, 1152, 1152], P(None, 'fsdp')
- b_proj: bfloat16 [2, 1152], replicated
- w_fc1: bfloat16 [2, 1152, 4608], P(None, 'fsdp')
- b_fc1: bfloat16 [2, 4608], replicated
- w_fc2: bfloat16 [2, 4608, 1152], P(None, 'fsdp')
- b_fc2: bfloat16 [2, 1152], replicated
Outputs:
- output: bfloat16 [2048, 16, 1152], P(('dp', 'fsdp'))
All inputs are finite; a program needn't handle non-finite values.
Results may differ from the reference program's by a relative error of at most 0.0162659.
Values are sent between devices in bfloat16 or wider.
A program may use at most 768 MiB of HBM per device.

```python
import jax
import jax.numpy as jnp
from jax import lax

SAMPLES = 64
GROUP_SIZE = 32
HIDDEN = 1152
TOKENS = 16
HEADS = 16
LAYERS = 2
BATCH = GROUP_SIZE * SAMPLES
HEAD_DIM = HIDDEN // HEADS
MLP_DIM = 4 * HIDDEN
LN_EPS = 1e-6


def setup_inputs(seed: int = 0, part: int = 0) -> dict:
    base_key = jax.random.key(seed)
    part_key = jax.random.fold_in(base_key, part)
    key_lat, key_cond = jax.random.split(part_key, 2)
    weight_keys = jax.random.split(jax.random.key(seed + 1), 10)

    def draw_weight(key_weight, fan_in, fan_out):
        return (jax.random.normal(key_weight, (LAYERS, fan_in, fan_out), jnp.float32) * fan_in ** -0.5).astype(jnp.bfloat16)

    def draw_bias(key_bias, fan_out):
        return (0.3 * jax.random.normal(key_bias, (LAYERS, fan_out), jnp.float32)).astype(jnp.bfloat16)

    return {
        'latents': jax.random.normal(key_lat, (BATCH, TOKENS, HIDDEN), jnp.float32).astype(jnp.bfloat16),
        'cond_emb': jax.random.normal(key_cond, (BATCH, HIDDEN), jnp.float32).astype(jnp.bfloat16),
        'w_ada': draw_weight(weight_keys[0], HIDDEN, 6 * HIDDEN),
        'b_ada': draw_bias(weight_keys[1], 6 * HIDDEN),
        'w_qkv': draw_weight(weight_keys[2], HIDDEN, 3 * HIDDEN),
        'b_qkv': draw_bias(weight_keys[3], 3 * HIDDEN),
        'w_proj': draw_weight(weight_keys[4], HIDDEN, HIDDEN),
        'b_proj': draw_bias(weight_keys[5], HIDDEN),
        'w_fc1': draw_weight(weight_keys[6], HIDDEN, MLP_DIM),
        'b_fc1': draw_bias(weight_keys[7], MLP_DIM),
        'w_fc2': draw_weight(weight_keys[8], MLP_DIM, HIDDEN),
        'b_fc2': draw_bias(weight_keys[9], HIDDEN),
    }


def layer_norm(values_in):
    mean_val = jnp.mean(values_in, axis=-1, keepdims=True)
    centered = values_in - mean_val
    var_val = jnp.mean(centered * centered, axis=-1, keepdims=True)
    return centered * lax.rsqrt(var_val + LN_EPS)


def dit_block(tokens_in, cond_act, weights):
    w_ada, b_ada, w_qkv, b_qkv, w_proj, b_proj, w_fc1, b_fc1, w_fc2, b_fc2 = weights
    modulation = jnp.dot(cond_act[None, :], w_ada, preferred_element_type=jnp.float32)[0] + b_ada.astype(jnp.float32)
    modulation = modulation.astype(jnp.bfloat16).astype(jnp.float32)
    shift_a, scale_a, gate_a, shift_m, scale_m, gate_m = jnp.split(modulation, 6)
    resid_a = tokens_in.astype(jnp.float32)
    normed = (layer_norm(resid_a) * (1.0 + scale_a) + shift_a).astype(jnp.bfloat16)
    qkv_rows = (jnp.dot(normed, w_qkv, preferred_element_type=jnp.float32) + b_qkv.astype(jnp.float32)).astype(jnp.bfloat16)
    qkv_rows = qkv_rows.astype(jnp.float32).reshape(TOKENS, 3, HEADS, HEAD_DIM)
    scores = jnp.einsum('qhd,khd->hqk', qkv_rows[:, 0], qkv_rows[:, 1]) * (HEAD_DIM ** -0.5)
    attn_probs = jax.nn.softmax(scores, axis=-1).astype(jnp.bfloat16).astype(jnp.float32)
    attn_out = jnp.einsum('hqk,khd->qhd', attn_probs, qkv_rows[:, 2]).astype(jnp.bfloat16).reshape(TOKENS, HIDDEN)
    proj_out = jnp.dot(attn_out, w_proj, preferred_element_type=jnp.float32) + b_proj.astype(jnp.float32)
    resid_b = (resid_a + gate_a * proj_out).astype(jnp.bfloat16).astype(jnp.float32)
    normed_b = (layer_norm(resid_b) * (1.0 + scale_m) + shift_m).astype(jnp.bfloat16)
    pre_act = jnp.dot(normed_b, w_fc1, preferred_element_type=jnp.float32) + b_fc1.astype(jnp.float32)
    hidden_act = jax.nn.gelu(pre_act, approximate=True).astype(jnp.bfloat16)
    mlp_out = jnp.dot(hidden_act, w_fc2, preferred_element_type=jnp.float32) + b_fc2.astype(jnp.float32)
    return (resid_b + gate_m * mlp_out).astype(jnp.bfloat16)


def reference(latents, cond_emb, w_ada, b_ada, w_qkv, b_qkv, w_proj, b_proj, w_fc1, b_fc1, w_fc2, b_fc2):
    stacked = (w_ada, b_ada, w_qkv, b_qkv, w_proj, b_proj, w_fc1, b_fc1, w_fc2, b_fc2)

    def one_sample(sample_pair):
        tokens_in, cond_row = sample_pair
        cond_act = jax.nn.silu(cond_row.astype(jnp.float32)).astype(jnp.bfloat16)

        def layer_step(carry_tok, weights):
            return dit_block(carry_tok, cond_act, weights), None

        result, _ = lax.scan(layer_step, tokens_in, stacked)
        return result

    return lax.map(one_sample, (latents, cond_emb))
```

```python
import functools
import math

import jax
import jax.numpy as jnp
from jax import lax
from jax.experimental import pallas as pl
from jax.experimental.pallas import tpu as pltpu
from jax.sharding import PartitionSpec as P

NUM_HEADS = 16
LN_EPS = 1e-6
MESH = pl.DeviceIdType.MESH
BF16 = jnp.bfloat16
F32 = jnp.float32


class Gather:
    COLS = (0, -1, 1, 2)

    def __init__(self, side, dst, unit_rows, kinds, send, recv, dsend, drecv, lsem):
        self.side, self.dst, self.unit, self.kinds = side, dst, unit_rows, kinds
        self.send, self.recv, self.dsend, self.drecv, self.lsem = send, recv, dsend, drecv, lsem
        me = lax.axis_index("fsdp")
        self.core = me % 2
        self.x = (me // 2) % side
        self.y = me // (2 * side)
        self.rows = unit_rows // (side * side)

    def chip(self, core, f, g):
        x = (self.x + f * (1 - core) + g * core + self.side) % self.side
        y = (self.y + f * core + g * (1 - core) + self.side) % self.side
        return y * self.side + x

    def dev(self, f, g):
        return {"fsdp": self.chip(self.core, f, g) * 2 + self.core}

    def partner(self):
        return {"fsdp": self.chip(self.core, 0, 0) * 2 + 1 - self.core}

    def piece(self, k, core, f, g):
        pairs, first, last = self.kinds
        chip = self.chip(core, f, g)
        layer, kk = k // pairs, k % pairs
        own_order = kk // first - kk // last
        count = last - first
        plain = (2 * kk + core) * self.unit + chip * self.rows
        ordered = 2 * first * self.unit + ((chip * 2 + core) * count + kk - first) * self.rows
        row = layer * (2 * pairs * self.unit) + (1 - own_order) * plain + own_order * ordered
        return self.dst.at[pl.ds(pl.multiple_of(row, 8), self.rows), :]

    def offsets(self, tag):
        if tag == 15:
            return 0, 0
        if tag < 3:
            return (-1, 1, 2)[tag], 0
        r, w = divmod(tag - 3, 3)
        return self.COLS[r], (-1, 1, 2)[w]

    def barrier(self):
        sem = pltpu.get_barrier_semaphore()
        peers = [self.dev(1, 0), self.dev(-1, 0), self.dev(0, 1), self.dev(0, -1), self.partner()]
        for p in peers:
            pl.semaphore_signal(sem, inc=1, device_id=p, device_id_type=MESH)
        pl.semaphore_wait(sem, len(peers))

    def copy(self, k, tag, src, f, g, to):
        return pltpu.make_async_remote_copy(
            src_ref=src, dst_ref=self.piece(k, self.core, f, g), send_sem=self.send.at[k, tag],
            recv_sem=self.recv.at[k, tag], device_id=to, device_id_type=MESH)

    def dcopy(self, k, tag, src, f, g, core=None):
        return pltpu.make_async_remote_copy(
            src_ref=src, dst_ref=self.piece(k, self.core if core is None else core, f, g),
            send_sem=self.dsend.at[k, tag], recv_sem=self.drecv.at[k, tag], device_id=self.partner(),
            device_id_type=MESH)

    def got(self, k, tag):
        f, g = self.offsets(tag)
        p = self.piece(k, self.core, f, g)
        self.copy(k, tag, p, f, g, self.partner()).wait_recv()
        self.dcopy(k, tag, p, f, g).start()
        return p

    def spread2(self, k, r, src):
        f = self.COLS[r]
        self.copy(k, 3 + 3 * r, src, f, 0, self.dev(0, 1)).start()
        self.copy(k, 4 + 3 * r, src, f, 0, self.dev(0, -1)).start()

    def ring2(self, k, r):
        d = 1 - 2 * ((k + r) % 2)
        self.got(k, 3 + 3 * r)
        self.got(k, 4 + 3 * r)
        f = self.COLS[r]
        self.copy(k, 5 + 3 * r, self.piece(k, self.core, f, -d), f, -d, self.dev(0, d)).start()

    def e0(self, k, own):
        self.copy(k, 0, own, 0, 0, self.dev(1, 0)).start()
        self.copy(k, 1, own, 0, 0, self.dev(-1, 0)).start()
        self.spread2(k, 0, own)
        self.dcopy(k, 15, own, 0, 0).start()
        pltpu.make_async_copy(own, self.piece(k, self.core, 0, 0), self.lsem.at[k]).start()

    def e1(self, k):
        d = 1 - 2 * (k % 2)
        p0 = self.got(k, 0)
        p1 = self.got(k, 1)
        self.copy(k, 2, self.piece(k, self.core, -d, 0), -d, 0, self.dev(d, 0)).start()
        self.spread2(k, 1, p0)
        self.spread2(k, 2, p1)

    def e2(self, k):
        self.ring2(k, 0)
        self.spread2(k, 3, self.got(k, 2))

    def e3(self, k):
        self.ring2(k, 1)
        self.ring2(k, 2)
        self.got(k, 5)

    def e4(self, k):
        self.ring2(k, 3)
        self.got(k, 8)
        self.got(k, 11)

    def e5(self, k):
        self.got(k, 14)

    def e6(self, k):
        for tag in range(16):
            f, g = self.offsets(tag)
            p = self.piece(k, 1 - self.core, f, g)
            q = self.piece(k, self.core, f, g)
            self.dcopy(k, tag, p, f, g, 1 - self.core).wait_recv()
            self.dcopy(k, tag, q, f, g).wait_send()
            if tag < 15:
                self.copy(k, tag, q, f, g, self.partner()).wait_send()
        own = self.piece(k, self.core, 0, 0)
        pltpu.make_async_copy(own, own, self.lsem.at[k]).wait()


def normed(v):
    c = v - jnp.mean(v, axis=-1, keepdims=True)
    return c * lax.rsqrt(jnp.mean(c * c, axis=-1, keepdims=True) + LN_EPS)


def blocks_kernel(side, layers, tokens, cond_ref, x_ref, bias_ref, ada_ref, qkvw_ref, proj_ref, fc1_ref, fc2_ref, out_ref,
                  gw, act, mods, u, qkv, h, acc, wslot, f2, mask, s_ref, wsem, f2sem, *sems):
    rows, hidden = out_ref.shape
    heads, dim = NUM_HEADS, hidden // NUM_HEADS
    hk = heads * tokens
    pairs, first, last = 9, 5, 7
    n = layers * pairs
    gat = Gather(side, gw, hidden, (pairs, first, last), *sems)
    core, piece_rows = gat.core, gat.rows

    gat.barrier()

    def start_pair(k):
        layer, kk = k // pairs, k % pairs

        def send(cond, ref, col, row=0):
            @pl.when(cond)
            def _():
                own = ref.at[layer, pl.ds(pl.multiple_of(row, 8), piece_rows),
                             pl.ds(pl.multiple_of(col * hidden, 128), hidden)]
                gat.e0(k, own)

        send(kk < 3, ada_ref, 2 * kk + core)
        send(kk == 3, qkvw_ref, core)
        send(jnp.logical_and(kk == 4, core == 0), qkvw_ref, 2)
        send(jnp.logical_and(kk == 4, core == 1), proj_ref, 0)
        send(jnp.logical_and(kk >= 5, kk < 7), fc2_ref, 0, (kk - 5) * piece_rows)
        send(kk >= 7, fc1_ref, 2 * (kk - 7) + core)

    def load_pair(c):
        return pltpu.make_async_copy(gw.at[pl.ds(pl.multiple_of(2 * c * hidden, 8), 2 * hidden), :],
                                     wslot.at[(c % pairs) % 3], wsem.at[(c % pairs) % 3])

    def load_f2(c):
        row = (c // pairs) * (2 * pairs * hidden) + 2 * first * hidden
        return pltpu.make_async_copy(gw.at[pl.ds(pl.multiple_of(row, 8), 4 * hidden), :], f2, f2sem.at[0])

    def fill_mask():
        lane = lax.broadcasted_iota(jnp.int32, (hk, hidden), 1)
        row = lax.broadcasted_iota(jnp.int32, (hk, hidden), 0)
        lo = (row // tokens) * dim
        mask[...] = jnp.where(jnp.logical_and(lane >= lo, lane < lo + dim), 1.0, 0.0).astype(BF16)

    def loop(size, step, fn, unroll=1):
        def it(i, carry):
            fn(pl.multiple_of(i * step, step))
            return carry
        lax.fori_loop(0, size // step, it, 0, unroll=unroll)

    def wide(j, r, size):
        v = mods[j, pl.ds(pl.multiple_of(r // tokens, 8), size // tokens), :]
        return jnp.broadcast_to(v[:, None, :], (size // tokens, tokens, hidden)).reshape(size, hidden)

    def weight(kk, half):
        return wslot[kk % 3, half * hidden:(half + 1) * hidden, :]

    def bias(l, i):
        return bias_ref[l, i:i + 1, :]

    def modulation(l, kk):
        for half in (0, 1):
            j = 2 * kk + half
            d = jnp.dot(act[...], weight(kk, half), preferred_element_type=F32)
            mods[j] = (d + bias(l, j)).astype(BF16).astype(F32)

    LB, MB = 128, 256

    def norm_to_u(shift, scale):
        def fn(r):
            v = normed(out_ref[pl.ds(r, LB), :].astype(F32))
            u[pl.ds(r, LB), :] = (v * (1.0 + wide(scale, r, LB)) + wide(shift, r, LB)).astype(BF16)
        loop(rows, LB, fn)

    def project(l, j, kk, half):
        def fn(r):
            d = jnp.dot(u[pl.ds(r, MB), :], weight(kk, half), preferred_element_type=F32)
            qkv[j, pl.ds(r, MB), :] = (d + bias(l, 6 + j)).astype(BF16)
        loop(rows, MB, fn)

    def expand(kv):
        return jnp.broadcast_to(kv[None], (heads, tokens, hidden)).reshape(hk, hidden) * mask[...]

    def scores(half):
        def fn(r):
            r = r + half * (rows // 2)
            q = qkv[0, pl.ds(r, tokens), :]
            k = qkv[1, pl.ds(r, tokens), :]
            s_ref[pl.ds(r, tokens), :] = lax.dot_general(q, expand(k), (((1,), (1,)), ((), ())),
                                                         preferred_element_type=F32)
        loop(rows // 2, tokens, fn, unroll=4)

    def softmax():
        blk = 64

        def segment(v, op, lane_id):
            for sh in (8, 4, 2, 1):
                up, down = pltpu.roll(v, hk - sh, 1), pltpu.roll(v, sh, 1)
                v = op(v, jnp.where((lane_id // sh) % 2 == 0, up, down))
            return v

        def fn(r):
            lane_id = lax.broadcasted_iota(jnp.int32, (blk, hk), 1)
            s = s_ref[pl.ds(r, blk), :] * (dim ** -0.5)
            e = jnp.exp(s - segment(s, jnp.maximum, lane_id))
            s_ref[pl.ds(r, blk), :] = e / segment(e, jnp.add, lane_id)
        loop(rows, blk, fn)

    def values(half):
        def fn(r):
            r = r + half * (rows // 2)
            v = qkv[2, pl.ds(r, tokens), :]
            p = s_ref[pl.ds(r, tokens), :].astype(BF16)
            u[pl.ds(r, tokens), :] = jnp.dot(p, expand(v), preferred_element_type=F32).astype(BF16)
        loop(rows // 2, tokens, fn, unroll=4)

    def out_proj(l):
        def fn(r):
            d = jnp.dot(u[pl.ds(r, MB), :], weight(4, 1), preferred_element_type=F32) + bias(l, 9)
            x = out_ref[pl.ds(r, MB), :].astype(F32)
            out_ref[pl.ds(r, MB), :] = (x + wide(2, r, MB) * d).astype(BF16)
        loop(rows, MB, fn)

    def fc1(l, g):
        def fn(r):
            d = jnp.dot(u[pl.ds(r, MB), :], weight(7 + g // 2, g % 2), preferred_element_type=F32) + bias(l, 10 + g)
            h[pl.ds(r, MB), :] = jax.nn.gelu(d, approximate=True).astype(BF16)
        loop(rows, MB, fn)

    def fc2(l, g):
        def fn(r):
            d = jnp.dot(h[pl.ds(r, MB), :], f2[g * hidden:(g + 1) * hidden, :], preferred_element_type=F32)
            if g > 0:
                d = acc[pl.ds(r, MB), :] + d
            if g < 3:
                acc[pl.ds(r, MB), :] = d
            else:
                x = out_ref[pl.ds(r, MB), :].astype(F32)
                out_ref[pl.ds(r, MB), :] = (x + wide(5, r, MB) * (d + bias(l, 14))).astype(BF16)
        loop(rows, MB, fn)

    plan = {
        (0, 0): [("prev", lambda l: fc1(l, 2))], (0, 1): [("", lambda l: modulation(l, 0))],
        (0, 2): [("prev", lambda l: fc2(l, 2))],
        (1, 0): [("prev", lambda l: fc1(l, 3))], (1, 1): [("", lambda l: modulation(l, 1))],
        (1, 2): [("prev", lambda l: fc2(l, 3))],
        (2, 1): [("", lambda l: modulation(l, 2))], (2, 2): [("", lambda l: norm_to_u(0, 1))],
        (3, 1): [("", lambda l: project(l, 0, 3, 0))], (3, 2): [("", lambda l: project(l, 1, 3, 1))],
        (4, 0): [("", lambda l: scores(0))], (4, 1): [("", lambda l: project(l, 2, 4, 0))],
        (4, 2): [("", lambda l: scores(1))],
        (5, 0): [("", lambda l: softmax())], (5, 1): [("", lambda l: values(0))], (5, 2): [("", lambda l: values(1))],
        (6, 0): [("", lambda l: out_proj(l))], (6, 1): [("", lambda l: norm_to_u(3, 4))],
        (7, 1): [("", lambda l: fc1(l, 0))], (7, 2): [("", lambda l: fc2(l, 0))],
        (8, 1): [("", lambda l: fc1(l, 1))], (8, 2): [("", lambda l: fc2(l, 1))],
    }

    def compute(c, part):
        layer, kk = c // pairs, c % pairs
        for (pair, when), tasks in plan.items():
            if when != part:
                continue
            for mark, task in tasks:
                if mark:
                    cond = jnp.logical_and(kk == pair, c >= pairs)
                    cl = layer - 1
                else:
                    cond = jnp.logical_and(kk == pair, jnp.logical_and(c >= 0, c < n))
                    cl = layer

                @pl.when(cond)
                def _(task=task, cl=cl):
                    task(cl)

    def within(k, fn):
        @pl.when(jnp.logical_and(k >= 0, k < n))
        def _():
            fn(k)

    lag = 4

    def plain(c):
        kk = c % pairs
        return jnp.logical_and(jnp.logical_and(c >= 0, c < n), jnp.logical_or(kk < first, kk >= last))

    def step(t, carry):
        c = t - lag
        within(t, start_pair)
        within(t - 2, gat.e3)
        within(c, gat.e6)

        @pl.when(plain(c))
        def _():
            load_pair(c).start()

        @pl.when(jnp.logical_and(c % pairs == last - 1, jnp.logical_and(c >= 0, c < n)))
        def _():
            load_f2(c).start()

        @pl.when(t == 0)
        def _():
            fill_mask()
            v = cond_ref[...].astype(F32)
            act[...] = jax.nn.silu(v).astype(BF16)
            out_ref[...] = x_ref[...]

        compute(c, 0)
        within(t - 1, gat.e2)
        within(t - 3, gat.e5)

        @pl.when(plain(c))
        def _():
            load_pair(c).wait()

        @pl.when(jnp.logical_and(c % pairs == last, jnp.logical_and(c >= 0, c < n)))
        def _():
            load_f2(c).wait()

        compute(c, 1)
        within(t, gat.e1)
        within(t - 2, gat.e4)
        compute(c, 2)
        return carry

    lax.fori_loop(0, n + lag + 2, step, 0)


def run_blocks(side, cond, x, bias, ada, qkvw, proj, fc1, fc2, tokens):
    rows, hidden = x.shape
    layers = ada.shape[0]
    n = layers * 9
    vm = pl.BlockSpec(memory_space=pltpu.VMEM)
    hk = NUM_HEADS * tokens
    dma = pltpu.SemaphoreType.DMA
    out, _ = pl.pallas_call(
        functools.partial(blocks_kernel, side, layers, tokens),
        out_shape=(jax.ShapeDtypeStruct((rows, hidden), BF16), jax.ShapeDtypeStruct((2 * n * hidden, hidden), BF16)),
        in_specs=[vm] * 8,
        out_specs=(vm, pl.BlockSpec(memory_space=pl.ANY)),
        scratch_shapes=[
            pltpu.VMEM(cond.shape, BF16), pltpu.VMEM((6,) + cond.shape, F32), pltpu.VMEM((rows, hidden), BF16),
            pltpu.VMEM((3, rows, hidden), BF16), pltpu.VMEM((rows, hidden), BF16), pltpu.VMEM((rows, hidden), F32),
            pltpu.VMEM((3, 2 * hidden, hidden), BF16), pltpu.VMEM((4 * hidden, hidden), BF16),
            pltpu.VMEM((hk, hidden), BF16), pltpu.VMEM((rows, hk), F32), dma((3,)), dma((1,)),
            dma((n, 15)), dma((n, 15)), dma((n, 16)), dma((n, 16)), dma((n,)),
        ],
        compiler_params=pltpu.CompilerParams(collective_id=0, has_side_effects=True, vmem_limit_bytes=67043328),
        name="dit_blocks",
    )(cond, x, bias, ada, qkvw, proj, fc1, fc2)
    return out


def solution(mesh):
    n_dev = mesh.shape["fsdp"]
    side = math.isqrt(n_dev // 2)
    batch_spec = P(("dp", "fsdp"), None, None)
    cond_spec = P(("dp", "fsdp"), None)
    shard_spec = P(None, "fsdp", None)
    bias_spec = P(None, None)

    def local_run(latents, cond_emb, w_ada, b_ada, w_qkv, b_qkv, w_proj, b_proj, w_fc1, b_fc1, w_fc2, b_fc2):
        samples, tokens, hidden = latents.shape
        layers = w_ada.shape[0]
        core = lax.axis_index("fsdp") % 2
        swap = [(i, i + 1 - 2 * (i % 2)) for i in range(n_dev)]

        def both(w):
            other = lax.ppermute(w, "fsdp", swap)
            return jnp.concatenate([jnp.where(core == 0, w, other), jnp.where(core == 0, other, w)], axis=1)

        bias = jnp.concatenate([b.astype(F32).reshape(layers, -1, hidden) for b in (b_ada, b_qkv, b_proj, b_fc1, b_fc2)],
                               axis=1)
        out = run_blocks(side, cond_emb, latents.reshape(samples * tokens, hidden), bias, both(w_ada), both(w_qkv),
                         both(w_proj), both(w_fc1), w_fc2, tokens)
        return out.reshape(latents.shape)

    in_specs = (batch_spec, cond_spec, shard_spec, bias_spec, shard_spec, bias_spec, shard_spec, bias_spec, shard_spec,
                bias_spec, shard_spec, bias_spec)
    return jax.shard_map(local_run, mesh=mesh, in_specs=in_specs, out_specs=batch_spec, check_vma=False)
```

```python
import functools
import math

import jax
import jax.numpy as jnp
from jax import lax
from jax.experimental import pallas as pl
from jax.experimental.pallas import tpu as pltpu
from jax.sharding import PartitionSpec as P

NUM_HEADS = 16
LN_EPS = 1e-6
MESH = pl.DeviceIdType.MESH
BF16 = jnp.bfloat16
F32 = jnp.float32


class Gather:
    COLS = (0, -1, 1, 2)

    def __init__(self, side, dst, unit_rows, kinds, send, recv, dsend, drecv, lsem):
        self.side, self.dst, self.unit, self.kinds = side, dst, unit_rows, kinds
        self.send, self.recv, self.dsend, self.drecv, self.lsem = send, recv, dsend, drecv, lsem
        me = lax.axis_index("fsdp")
        self.core = me % 2
        self.x = (me // 2) % side
        self.y = me // (2 * side)
        self.rows = unit_rows // (side * side)

    def chip(self, core, f, g):
        x = (self.x + f * (1 - core) + g * core + self.side) % self.side
        y = (self.y + f * core + g * (1 - core) + self.side) % self.side
        return y * self.side + x

    def dev(self, f, g):
        return {"fsdp": self.chip(self.core, f, g) * 2 + self.core}

    def at(self, chip, core):
        return {"fsdp": chip * 2 + core}

    def partner(self):
        return {"fsdp": self.chip(self.core, 0, 0) * 2 + 1 - self.core}

    def piece(self, k, core, f, g):
        pairs, first, last = self.kinds
        chip = self.chip(core, f, g)
        layer, kk = k // pairs, k % pairs
        own_order = kk // first - 2 * (kk // last)
        count = last - first
        plain = (2 * kk + core) * self.unit + chip * self.rows
        ordered = 2 * first * self.unit + ((chip * 2 + core) * count + kk - first) * self.rows
        row = layer * (2 * pairs * self.unit) + (1 - own_order) * plain + own_order * ordered
        return self.dst.at[pl.ds(pl.multiple_of(row, 8), self.rows), :]

    def offsets(self, tag):
        if tag == 15:
            return 0, 0
        if tag < 3:
            return (-1, 1, 2)[tag], 0
        r, w = divmod(tag - 3, 3)
        return self.COLS[r], (-1, 1, 2)[w]

    def barrier(self):
        sem = pltpu.get_barrier_semaphore()
        peers = [self.partner()]
        for core in (0, 1):
            peers += [self.at(self.chip(way, o, 0), core) for way in (0, 1) for o in range(1, self.side)]
        for p in peers:
            pl.semaphore_signal(sem, inc=1, device_id=p, device_id_type=MESH)
        pl.semaphore_wait(sem, len(peers))

    def copy(self, k, tag, src, f, g, to):
        return pltpu.make_async_remote_copy(
            src_ref=src, dst_ref=self.piece(k, self.core, f, g), send_sem=self.send.at[k, tag],
            recv_sem=self.recv.at[k, tag], device_id=to, device_id_type=MESH)

    def dcopy(self, k, tag, src, f, g, core=None):
        return pltpu.make_async_remote_copy(
            src_ref=src, dst_ref=self.piece(k, self.core if core is None else core, f, g),
            send_sem=self.dsend.at[k, tag], recv_sem=self.drecv.at[k, tag], device_id=self.partner(),
            device_id_type=MESH)

    def got(self, k, tag):
        f, g = self.offsets(tag)
        p = self.piece(k, self.core, f, g)
        self.copy(k, tag, p, f, g, self.partner()).wait_recv()
        self.dcopy(k, tag, p, f, g).start()
        return p

    def spread2(self, k, r, src):
        f = self.COLS[r]
        self.copy(k, 3 + 3 * r, src, f, 0, self.dev(0, 1)).start()
        self.copy(k, 4 + 3 * r, src, f, 0, self.dev(0, -1)).start()

    def ring2(self, k, r):
        d = 1 - 2 * ((k + r) % 2)
        self.got(k, 3 + 3 * r)
        self.got(k, 4 + 3 * r)
        f = self.COLS[r]
        self.copy(k, 5 + 3 * r, self.piece(k, self.core, f, -d), f, -d, self.dev(0, d)).start()

    def e0(self, k, own):
        self.copy(k, 0, own, 0, 0, self.dev(1, 0)).start()
        self.copy(k, 1, own, 0, 0, self.dev(-1, 0)).start()
        self.spread2(k, 0, own)
        self.dcopy(k, 15, own, 0, 0).start()
        pltpu.make_async_copy(own, self.piece(k, self.core, 0, 0), self.lsem.at[k]).start()

    def e1(self, k):
        d = 1 - 2 * (k % 2)
        p0 = self.got(k, 0)
        p1 = self.got(k, 1)
        self.copy(k, 2, self.piece(k, self.core, -d, 0), -d, 0, self.dev(d, 0)).start()
        self.spread2(k, 1, p0)
        self.spread2(k, 2, p1)

    def e2(self, k):
        self.ring2(k, 0)
        self.spread2(k, 3, self.got(k, 2))

    def e3(self, k):
        self.ring2(k, 1)
        self.ring2(k, 2)
        self.got(k, 5)

    def e4(self, k):
        self.ring2(k, 3)
        self.got(k, 8)
        self.got(k, 11)

    def e5(self, k):
        self.got(k, 14)

    def e6(self, k):
        for tag in range(16):
            f, g = self.offsets(tag)
            p = self.piece(k, 1 - self.core, f, g)
            q = self.piece(k, self.core, f, g)
            self.dcopy(k, tag, p, f, g, 1 - self.core).wait_recv()
            self.dcopy(k, tag, q, f, g).wait_send()
            if tag < 15:
                self.copy(k, tag, q, f, g, self.partner()).wait_send()
        own = self.piece(k, self.core, 0, 0)
        pltpu.make_async_copy(own, own, self.lsem.at[k]).wait()


class Modulation:
    def __init__(self, gat, layers, ada, bias, cond, land, conds, act, made, mods, csem, crecv, asem, arecv, gsem, grecv,
                 msem, mrecv):
        self.gat, self.layers, self.ada, self.bias, self.cond = gat, layers, ada, bias, cond
        self.land, self.conds, self.act, self.made, self.mods = land, conds, act, made, mods
        self.csem, self.crecv, self.asem, self.arecv = csem, crecv, asem, arecv
        self.gsem, self.grecv, self.msem, self.mrecv = gsem, grecv, msem, mrecv
        self.side, self.core = gat.side, gat.core
        self.f = gat.x * (1 - gat.core) + gat.y * gat.core
        self.count = 3 * layers
        self.samples = cond.shape[0]

    def remote(self, src, dst, send, recv, to):
        return pltpu.make_async_remote_copy(src_ref=src, dst_ref=dst, send_sem=send, recv_sem=recv, device_id=to,
                                            device_id_type=MESH)

    def cond_slot(self, i):
        return self.conds.at[pl.ds(pl.multiple_of(i * self.samples, 16), self.samples), :]

    def rows_of(self, slot, f, g):
        row = slot * self.gat.unit + self.gat.chip(self.core, f, g) * self.gat.rows
        return self.land.at[pl.ds(pl.multiple_of(row, 8), self.gat.rows), :]

    def own(self, j):
        col = (2 * (j % 3) + self.core) * self.gat.unit
        return self.ada.at[j // 3, :, pl.ds(pl.multiple_of(col, 128), self.gat.unit)]

    def owned(self, fn):
        for slot in range(-(-self.count // self.side)):
            @pl.when(self.f + slot * self.side < self.count)
            def _(slot=slot):
                fn(slot)

    def a0(self):
        gat, side = self.gat, self.side
        pltpu.make_async_copy(self.cond, self.cond_slot(self.core), self.csem.at[0]).start()
        self.remote(self.cond, self.cond_slot(self.core), self.csem.at[1], self.crecv.at[self.core], gat.partner()).start()
        for way in (0, 1):
            for o in range(1, side):
                i = (side - o) * 2 + self.core
                self.remote(self.cond, self.cond_slot(i), self.csem.at[2 + way * side + o], self.crecv.at[i],
                            gat.at(gat.chip(way, o, 0), way)).start()
        for j in range(self.count):
            o = (j % side - self.f + side) % side
            dst = self.rows_of(j // side, 0, 0)

            @pl.when(o == 0)
            def _(j=j, dst=dst):
                pltpu.make_async_copy(self.own(j), dst, self.asem.at[j]).start()

            @pl.when(o != 0)
            def _(j=j, o=o, dst=dst):
                self.remote(self.own(j), dst, self.asem.at[j], self.arecv.at[j // side, (side - o) % side],
                            gat.dev(o, 0)).start()

    def ring(self, slot, r, w, f, g, to):
        p = self.rows_of(slot, f, g)
        i = 3 * r + w
        return self.remote(p, p, self.gsem.at[slot, i], self.grecv.at[slot, i], to)

    def a1(self):
        gat = self.gat

        def fn(slot):
            for r in range(self.side):
                p = self.rows_of(slot, r, 0)
                if r == 0:
                    pltpu.make_async_copy(p, p, self.asem.at[self.f + slot * self.side]).wait()
                else:
                    self.remote(p, p, self.asem.at[0], self.arecv.at[slot, r], gat.partner()).wait_recv()
                self.ring(slot, r, 0, r, 0, gat.dev(0, 1)).start()
                self.ring(slot, r, 1, r, 0, gat.dev(0, -1)).start()
        self.owned(fn)

    def a2(self):
        def fn(slot):
            for r in range(self.side):
                self.ring(slot, r, 0, r, -1, self.gat.partner()).wait_recv()
                self.ring(slot, r, 1, r, 1, self.gat.partner()).wait_recv()
                d = 1 - 2 * (r % 2)
                self.ring(slot, r, 2, r, -d, self.gat.dev(0, d)).start()
        self.owned(fn)

    def made_part(self, slot, i):
        return self.made.at[slot, pl.ds(pl.multiple_of(i * self.samples, 16), self.samples), :]

    def a3(self):
        gat, side, unit = self.gat, self.side, self.gat.unit
        people = 2 * side * self.samples
        pltpu.make_async_copy(self.cond, self.cond_slot(self.core), self.csem.at[0]).wait()
        for i in range(2 * side):
            @pl.when(self.core != i)
            def _(i=i):
                self.remote(self.cond, self.cond_slot(i), self.csem.at[1], self.crecv.at[i], gat.partner()).wait_recv()
        blk = people // 4

        def silu(b, carry):
            r = pl.multiple_of(b * blk, blk)
            self.act[pl.ds(r, blk), :] = jax.nn.silu(self.conds[pl.ds(r, blk), :].astype(F32)).astype(BF16)
            return carry
        lax.fori_loop(0, 4, silu, 0)

        def fn(slot):
            for r in range(side):
                self.ring(slot, r, 2, r, 2, gat.partner()).wait_recv()
            j = self.f + slot * side
            layer, i = j // 3, 2 * (j % 3) + self.core
            row = self.bias[layer, pl.ds(i, 1), :]

            def mul(b, carry):
                r = pl.multiple_of(b * blk, blk)
                d = jnp.dot(self.act[pl.ds(r, blk), :], self.land[slot * unit:(slot + 1) * unit, :],
                            preferred_element_type=F32)
                self.made[slot, pl.ds(r, blk), :] = (d + row).astype(BF16)
                return carry
            lax.fori_loop(0, 4, mul, 0)
            dst = self.mods.at[layer * 6 + i]
            sem = self.mrecv.at[layer * 6 + i]
            for o in range(side):
                for core in (0, 1):
                    q = 2 * o + core
                    src = self.made_part(slot, q)
                    if o:
                        self.remote(src, dst, self.msem.at[slot, q], sem, gat.at(gat.chip(self.core, o, 0), core)).start()
                    else:
                        @pl.when(self.core == core)
                        def _(src=src):
                            pltpu.make_async_copy(src, dst, sem).start()

                        @pl.when(self.core != core)
                        def _(src=src, q=q):
                            self.remote(src, dst, self.msem.at[slot, q], sem, gat.partner()).start()
        self.owned(fn)

    def a4(self):
        gat, side = self.gat, self.side
        for i in range(2 * self.count):
            m = self.mods.at[i]
            pltpu.make_async_copy(m, m, self.mrecv.at[i]).wait()
        c = self.cond
        self.remote(c, c, self.csem.at[1], self.crecv.at[0], gat.partner()).wait_send()
        for way in (0, 1):
            for o in range(1, side):
                self.remote(c, c, self.csem.at[2 + way * side + o], self.crecv.at[0], gat.partner()).wait_send()
        for j in range(self.count):
            @pl.when((j % side - self.f + side) % side != 0)
            def _(j=j):
                p = self.own(j)
                self.remote(p, p, self.asem.at[j], self.arecv.at[0, 0], gat.partner()).wait_send()

        def fn(slot):
            for r in range(side):
                for w in range(3):
                    self.ring(slot, r, w, r, 0, gat.partner()).wait_send()
            for q in range(2 * side):
                @pl.when(self.core != q)
                def _(q=q):
                    p = self.made_part(slot, q)
                    self.remote(p, p, self.msem.at[slot, q], self.mrecv.at[0], gat.partner()).wait_send()
        self.owned(fn)


def normed(v):
    c = v - jnp.mean(v, axis=-1, keepdims=True)
    return c * lax.rsqrt(jnp.mean(c * c, axis=-1, keepdims=True) + LN_EPS)


def blocks_kernel(side, layers, tokens, cond_ref, x_ref, bias_ref, ada_ref, qkvw_ref, proj_ref, fc1_ref, fc2_ref, out_ref,
                  gw, mods, u, qkv, h, acc, wslot, f2, mask, seg, s_ref, wsem, f2sem, *sems):
    rows, hidden = out_ref.shape
    heads, dim = NUM_HEADS, hidden // NUM_HEADS
    hk = heads * tokens
    pairs, first, last = 6, 2, 4
    n = layers * pairs
    gat = Gather(side, gw, hidden, (pairs, first, last), *sems[:5])
    core, piece_rows = gat.core, gat.rows
    mod = Modulation(gat, layers, ada_ref, bias_ref, cond_ref, wslot.at[2], u, h, qkv, mods, *sems[5:])

    gat.barrier()

    def start_pair(k):
        layer, kk = k // pairs, k % pairs

        def send(cond, ref, col, row=0):
            @pl.when(cond)
            def _():
                own = ref.at[layer, pl.ds(pl.multiple_of(row, 8), piece_rows),
                             pl.ds(pl.multiple_of(col * hidden, 128), hidden)]
                gat.e0(k, own)

        send(kk == 0, qkvw_ref, core)
        send(jnp.logical_and(kk == 1, core == 0), qkvw_ref, 2)
        send(jnp.logical_and(kk == 1, core == 1), proj_ref, 0)
        send(jnp.logical_and(kk >= first, kk < last), fc2_ref, 0, (kk - first) * piece_rows)
        send(kk >= last, fc1_ref, 2 * (kk - last) + core)

    def load_pair(c):
        return pltpu.make_async_copy(gw.at[pl.ds(pl.multiple_of(2 * c * hidden, 8), 2 * hidden), :],
                                     wslot.at[(c % pairs) % 3], wsem.at[(c % pairs) % 3])

    def load_f2(c):
        row = (c // pairs) * (2 * pairs * hidden) + 2 * first * hidden
        return pltpu.make_async_copy(gw.at[pl.ds(pl.multiple_of(row, 8), 4 * hidden), :], f2, f2sem.at[0])

    def fill_mask():
        lane = lax.broadcasted_iota(jnp.int32, (hk, hidden), 1)
        row = lax.broadcasted_iota(jnp.int32, (hk, hidden), 0)
        lo = (row // tokens) * dim
        mask[...] = jnp.where(jnp.logical_and(lane >= lo, lane < lo + dim), 1.0, 0.0).astype(BF16)
        head = [lax.broadcasted_iota(jnp.int32, (hk, hk), d) // tokens for d in (0, 1)]
        seg[...] = jnp.where(head[0] == head[1], 1.0, 0.0).astype(BF16)

    def loop(size, step, fn, unroll=1):
        def it(i, carry):
            fn(pl.multiple_of(i * step, step))
            return carry
        lax.fori_loop(0, size // step, it, 0, unroll=unroll)

    def wide(l, j, r, size):
        v = mods[6 * l + j, pl.ds(pl.multiple_of(r // tokens, 16), size // tokens), :].astype(F32)
        return jnp.broadcast_to(v[:, None, :], (size // tokens, tokens, hidden)).reshape(size, hidden)

    def weight(kk, half):
        return wslot[kk % 3, half * hidden:(half + 1) * hidden, :]

    def bias(l, i):
        return bias_ref[l, i:i + 1, :]

    LB, MB = 256, 256

    def norm_to_u(l, shift, scale):
        def fn(r):
            v = normed(out_ref[pl.ds(r, LB), :].astype(F32))
            u[pl.ds(r, LB), :] = (v * (1.0 + wide(l, scale, r, LB)) + wide(l, shift, r, LB)).astype(BF16)
        loop(rows, LB, fn)

    def project(l, j, kk, half):
        def fn(r):
            d = jnp.dot(u[pl.ds(r, MB), :], weight(kk, half), preferred_element_type=F32)
            qkv[j, pl.ds(r, MB), :] = (d + bias(l, 6 + j)).astype(BF16)
        loop(rows, MB, fn)

    def expand(kv):
        return jnp.broadcast_to(kv[None], (heads, tokens, hidden)).reshape(hk, hidden) * mask[...]

    def scores(half):
        def fn(r):
            r = r + half * (rows // 2)
            q = qkv[0, pl.ds(r, tokens), :]
            k = qkv[1, pl.ds(r, tokens), :]
            s_ref[pl.ds(r, tokens), :] = lax.dot_general(q, expand(k), (((1,), (1,)), ((), ())),
                                                         preferred_element_type=F32)
        loop(rows // 2, tokens, fn, unroll=4)

    def softmax():
        blk = 256

        def fn(r):
            even = [(lax.broadcasted_iota(jnp.int32, (blk, hk), 1) // sh) % 2 == 0 for sh in (8, 4, 2, 1)]
            v = s_ref[pl.ds(r, blk), :] * (dim ** -0.5)
            top = v
            for sh, cond in zip((8, 4, 2, 1), even):
                top = jnp.maximum(top, jnp.where(cond, pltpu.roll(top, hk - sh, 1), pltpu.roll(top, sh, 1)))
            e = jnp.exp(v - top)
            total, rest = 0.0, e
            for _ in range(3):
                part = rest.astype(BF16)
                total = total + jnp.dot(part, seg[...], preferred_element_type=F32)
                rest = rest - part.astype(F32)
            s_ref[pl.ds(r, blk), :] = e / total
        loop(rows, blk, fn)

    def values(half):
        def fn(r):
            r = r + half * (rows // 2)
            v = qkv[2, pl.ds(r, tokens), :]
            p = s_ref[pl.ds(r, tokens), :].astype(BF16)
            u[pl.ds(r, tokens), :] = jnp.dot(p, expand(v), preferred_element_type=F32).astype(BF16)
        loop(rows // 2, tokens, fn, unroll=4)

    def out_proj(l):
        def fn(r):
            d = jnp.dot(u[pl.ds(r, MB), :], weight(1, 1), preferred_element_type=F32) + bias(l, 9)
            x = out_ref[pl.ds(r, MB), :].astype(F32)
            out_ref[pl.ds(r, MB), :] = (x + wide(l, 2, r, MB) * d).astype(BF16)
        loop(rows, MB, fn)

    def fc1(l, g):
        def fn(r):
            d = jnp.dot(u[pl.ds(r, MB), :], weight(last + g // 2, g % 2), preferred_element_type=F32) + bias(l, 10 + g)
            h[pl.ds(r, MB), :] = jax.nn.gelu(d, approximate=True).astype(BF16)
        loop(rows, MB, fn)

    def fc2(l, g):
        def fn(r):
            d = jnp.dot(h[pl.ds(r, MB), :], f2[g * hidden:(g + 1) * hidden, :], preferred_element_type=F32)
            if g > 0:
                d = acc[pl.ds(r, MB), :] + d
            if g < 3:
                acc[pl.ds(r, MB), :] = d
            else:
                x = out_ref[pl.ds(r, MB), :].astype(F32)
                out_ref[pl.ds(r, MB), :] = (x + wide(l, 5, r, MB) * (d + bias(l, 14))).astype(BF16)
        loop(rows, MB, fn)

    plan = {
        (0, 0): [("prev", lambda l: fc1(l, 3))],
        (0, 1): [("prev", lambda l: fc2(l, 3)), ("later", lambda l: norm_to_u(l, 0, 1))],
        (0, 2): [("", lambda l: project(l, 0, 0, 0))],
        (1, 0): [("", lambda l: project(l, 1, 0, 1))], (1, 1): [("", lambda l: scores(0))],
        (1, 2): [("", lambda l: scores(1))],
        (2, 0): [("", lambda l: project(l, 2, 1, 0))], (2, 1): [("", lambda l: softmax())],
        (2, 2): [("", lambda l: values(0))],
        (3, 0): [("", lambda l: values(1))], (3, 1): [("", lambda l: out_proj(l))],
        (3, 2): [("", lambda l: norm_to_u(l, 3, 4))],
        (4, 0): [("", lambda l: fc1(l, 0))], (4, 1): [("", lambda l: fc2(l, 0))], (4, 2): [("", lambda l: fc1(l, 1))],
        (5, 0): [("", lambda l: fc2(l, 1))], (5, 1): [("", lambda l: fc1(l, 2))], (5, 2): [("", lambda l: fc2(l, 2))],
    }

    def compute(c, part):
        layer, kk = c // pairs, c % pairs
        for (pair, when), tasks in plan.items():
            if when != part:
                continue
            for mark, task in tasks:
                if mark == "later":
                    cond = jnp.logical_and(kk == pair, jnp.logical_and(c >= pairs, c < n))
                    cl = layer
                elif mark:
                    cond = jnp.logical_and(kk == pair, c >= pairs)
                    cl = layer - 1
                else:
                    cond = jnp.logical_and(kk == pair, jnp.logical_and(c >= 0, c < n))
                    cl = layer

                @pl.when(cond)
                def _(task=task, cl=cl):
                    task(cl)

    def within(k, fn):
        @pl.when(jnp.logical_and(k >= 0, k < n))
        def _():
            fn(k)

    lag = 4

    def plain(c):
        kk = c % pairs
        return jnp.logical_and(jnp.logical_and(c >= 0, c < n), jnp.logical_or(kk < first, kk >= last))

    def step(t, carry):
        c = t - lag

        @pl.when(t == 0)
        def _():
            mod.a0()

        within(t, start_pair)
        within(t - 2, gat.e3)

        @pl.when(plain(c))
        def _():
            load_pair(c).wait()

        @pl.when(jnp.logical_and(c % pairs == last, jnp.logical_and(c >= 0, c < n)))
        def _():
            load_f2(c).wait()

        @pl.when(t == 1)
        def _():
            mod.a2()

        @pl.when(t == 3)
        def _():
            mod.a4()

        @pl.when(t == 0)
        def _():
            fill_mask()
            out_ref[...] = x_ref[...]

        compute(c, 0)
        within(t - 1, gat.e2)
        within(t - 3, gat.e5)

        @pl.when(t == 0)
        def _():
            mod.a1()

        @pl.when(t == 3)
        def _():
            norm_to_u(0, 0, 1)

        compute(c, 1)
        within(t, gat.e1)
        within(t - 2, gat.e4)
        within(t - 3, gat.e6)

        @pl.when(plain(c + 1))
        def _():
            load_pair(c + 1).start()

        @pl.when(jnp.logical_and((c + 1) % pairs == last - 1, jnp.logical_and(c + 1 >= 0, c + 1 < n)))
        def _():
            load_f2(c + 1).start()

        @pl.when(t == 1)
        def _():
            mod.a3()

        compute(c, 2)
        return carry

    lax.fori_loop(0, n + lag + 1, step, 0)


def run_blocks(side, cond, x, bias, ada, qkvw, proj, fc1, fc2, tokens):
    rows, hidden = x.shape
    layers = ada.shape[0]
    n = layers * 6
    slots = -(-3 * layers // side)
    vm = pl.BlockSpec(memory_space=pltpu.VMEM)
    hk = NUM_HEADS * tokens
    dma = pltpu.SemaphoreType.DMA
    out, _ = pl.pallas_call(
        functools.partial(blocks_kernel, side, layers, tokens),
        out_shape=(jax.ShapeDtypeStruct((rows, hidden), BF16), jax.ShapeDtypeStruct((2 * n * hidden, hidden), BF16)),
        in_specs=[vm] * 8,
        out_specs=(vm, pl.BlockSpec(memory_space=pl.ANY)),
        scratch_shapes=[
            pltpu.VMEM((6 * layers,) + cond.shape, BF16), pltpu.VMEM((rows, hidden), BF16),
            pltpu.VMEM((3, rows, hidden), BF16), pltpu.VMEM((rows, hidden), BF16), pltpu.VMEM((rows, hidden), F32),
            pltpu.VMEM((3, 2 * hidden, hidden), BF16), pltpu.VMEM((4 * hidden, hidden), BF16),
            pltpu.VMEM((hk, hidden), BF16), pltpu.VMEM((hk, hk), BF16), pltpu.VMEM((rows, hk), F32), dma((3,)), dma((1,)),
            dma((n, 15)), dma((n, 15)), dma((n, 16)), dma((n, 16)), dma((n,)),
            dma((2 + 2 * side,)), dma((2 * side,)), dma((3 * layers,)), dma((slots, side)), dma((slots, 3 * side)),
            dma((slots, 3 * side)), dma((slots, 2 * side)), dma((6 * layers,)),
        ],
        compiler_params=pltpu.CompilerParams(collective_id=0, has_side_effects=True, vmem_limit_bytes=67043328),
        name="dit_blocks",
    )(cond, x, bias, ada, qkvw, proj, fc1, fc2)
    return out


def solution(mesh):
    n_dev = mesh.shape["fsdp"]
    side = math.isqrt(n_dev // 2)
    batch_spec = P(("dp", "fsdp"), None, None)
    cond_spec = P(("dp", "fsdp"), None)
    shard_spec = P(None, "fsdp", None)
    bias_spec = P(None, None)

    def local_run(latents, cond_emb, w_ada, b_ada, w_qkv, b_qkv, w_proj, b_proj, w_fc1, b_fc1, w_fc2, b_fc2):
        samples, tokens, hidden = latents.shape
        layers = w_ada.shape[0]
        core = lax.axis_index("fsdp") % 2
        swap = [(i, i + 1 - 2 * (i % 2)) for i in range(n_dev)]

        def both(w):
            other = lax.ppermute(w, "fsdp", swap)
            return jnp.concatenate([jnp.where(core == 0, w, other), jnp.where(core == 0, other, w)], axis=1)

        bias = jnp.concatenate([b.astype(F32).reshape(layers, -1, hidden) for b in (b_ada, b_qkv, b_proj, b_fc1, b_fc2)],
                               axis=1)
        out = run_blocks(side, cond_emb, latents.reshape(samples * tokens, hidden), bias, both(w_ada), both(w_qkv),
                         both(w_proj), both(w_fc1), w_fc2, tokens)
        return out.reshape(latents.shape)

    in_specs = (batch_spec, cond_spec, shard_spec, bias_spec, shard_spec, bias_spec, shard_spec, bias_spec, shard_spec,
                bias_spec, shard_spec, bias_spec)
    return jax.shard_map(local_run, mesh=mesh, in_specs=in_specs, out_specs=batch_spec, check_vma=False)
```
